32 devices in a mesh: dp: 16 (over z, y, core), level: 2 (over x).
Axes of the slice: x: 2, y: 2, z: 4, core: 2. Of those that a mesh axis runs over, the one named last changes fastest.
Arguments:
- token_ids: int32 [16, 2, 1536], P('dp', 'level'), may hold values from 0 to 1023
- decoded_mask: int32 [16, 2, 1536], P('dp', 'level'), may hold values 0 or 1
- levels_done: int32 [16], P('dp'), may hold values from 0 to 1
- code_tables: bfloat16 [2, 1024, 1024], P('level'), may hold values from -6 to 6
- mask_vectors: bfloat16 [2, 1024], P('level'), may hold values from -6 to 6
- w_qkv: bfloat16 [3, 1024, 1024], P(None, 'dp', 'level'), may hold values from -6 to 6
- w_out: bfloat16 [1024, 1024], P('level', 'dp'), may hold values from -0.1875 to 0.1875
- w_expand: bfloat16 [1024, 2048], P('dp'), may hold values from -0.1875 to 0.1875
- w_depth: bfloat16 [5, 1024], replicated, may hold values from -2.5 to 2.5
- w_project: bfloat16 [1024, 1024], P('dp'), may hold values from -0.1875 to 0.1875
- level_heads: bfloat16 [2, 1024, 1024], P('level'), may hold values from -0.1875 to 0.1875
Outputs:
- logits: bfloat16 [16, 2, 1536, 1024], P('dp', 'level')
The draws below stay inside these ranges and needn't reach their ends.
Inputs may be any that keep to these rules, and one draw needn't show every extreme that they name: `levels_done`: levels below it are fully decoded; the level equal to it is the one being decoded.
All inputs are finite; a program needn't handle non-finite values. No bound on the sum of `decoded_mask` on one device may be relied on, other than what follows from the above.
Results may differ from the reference program's by a relative error of at most 0.006.
Values may be sent and summed in bfloat16 or wider, within the bound.
No kernel may reach another device: no remote copies, remote signals or barrier semaphores. Data moves between devices by JAX's collectives and lax.ppermute only.
A program may use at most 192 MiB of HBM per device.

```python
import jax
import jax.numpy as jnp
from jax import lax

D = 1024
HEADS = 16
VOCAB = 1024
FRAMES = 1536
KERNEL = 5
HEAD_DIM = 64
LEVELS = 2
CLIPS = 16


def draw_w_qkv(key, part):
    spread = D ** (-0.5)
    weights = jax.random.normal(jax.random.fold_in(key, 11), (3, D, D), jnp.float32) * spread
    weights = jnp.clip(weights, -6.0 * spread, 6.0 * spread)
    return jnp.clip(weights, -6.0, 6.0).astype(jnp.bfloat16)


def with_ends(values, key, low, top_value):
    longest = values.shape.index(max(values.shape))
    spots = []
    for shift in (0, 1):
        where = [jax.random.randint(jax.random.fold_in(key, axis), (), 0, length) for axis, length in enumerate(values.shape)]
        where[longest] = (where[longest] + shift) % values.shape[longest]
        spots.append(tuple(where))
    return values.at[spots[0]].set(low).at[spots[1]].set(top_value)


def block_scale(own_key, shape, split, low, top_value):
    gain = 1.0
    for dim, shards_of in split:
        steps = jax.random.uniform(jax.random.fold_in(jax.random.fold_in(own_key, 6), dim), (shards_of,), jnp.float32, low / len(split), top_value / len(split))
        gain = gain * jnp.repeat(jnp.exp(steps), shape[dim] // shards_of).reshape((-1,) + (1,) * (len(shape) - 1 - dim))
    return gain


def centred(stream_key, extent, width, bound, pieces=(), held_as=jnp.bfloat16):
    array = jax.random.normal(stream_key, extent, jnp.float32) * width
    if len(pieces) > 0:
        array = block_scale(stream_key, extent, pieces, -0.22, 0.18) * array
    return jnp.clip(array, min=-bound, max=bound).astype(held_as)


def setup_inputs(seed: int = 0) -> dict:
    streams_of = jax.random.split(jax.random.key(seed), 12)
    return {
        "token_ids": with_ends(jax.random.randint(streams_of[0], (CLIPS, LEVELS, FRAMES), 0, VOCAB), jax.random.fold_in(streams_of[0], 1), 0, VOCAB - 1).astype(jnp.int32),
        "decoded_mask": with_ends((jax.random.randint(streams_of[1], (CLIPS, LEVELS, FRAMES), 0, 2) < 1).astype(jnp.int32), jax.random.fold_in(streams_of[1], 1), 0, 1),
        "levels_done": with_ends(jax.random.randint(streams_of[2], (CLIPS,), 0, LEVELS), jax.random.fold_in(streams_of[2], 1), 0, LEVELS - 1).astype(jnp.int32),
        "code_tables": centred(streams_of[3], (LEVELS, VOCAB, D), 1.0, 6.0, ((0, 2),)),
        "mask_vectors": centred(streams_of[4], (LEVELS, D), 1.0, 6.0, ((0, 2),)),
        "w_qkv": draw_w_qkv(jax.random.fold_in(streams_of[11], 71), 0),
        "w_out": centred(streams_of[6], (D, D), D ** -0.5, 0.1875, ((0, 2), (1, 16))),
        "w_expand": centred(streams_of[7], (D, 2 * D), D ** -0.5, 0.1875, ((0, 16),)),
        "w_depth": centred(streams_of[8], (KERNEL, D), KERNEL ** -0.5, 2.5),
        "w_project": centred(streams_of[9], (D, D), D ** -0.5, 0.1875, ((0, 16),)),
        "level_heads": centred(streams_of[10], (LEVELS, D, VOCAB), D ** -0.5, 0.1875, ((0, 2),)),
    }


def layer_norm(values):
    centered = values - lax.optimization_barrier(jnp.mean(values, axis=-1, keepdims=True))
    variance = lax.optimization_barrier(jnp.mean(centered * centered, axis=-1, keepdims=True))
    return centered * lax.rsqrt(variance + 1e-05)

def clip_step(token_ids, decoded_mask, levels_done, code_tables, mask_vectors, w_qkv, w_out, w_expand, w_depth, w_project, level_heads):
    level_ids = jnp.arange(LEVELS, dtype=jnp.int32)[:, None]
    use_token = (level_ids < levels_done) | (level_ids == levels_done) & (decoded_mask == 1)
    picked = jax.vmap(lambda table_one, ids_one: jnp.take(table_one, ids_one, axis=0))(code_tables, token_ids.astype(jnp.int32)).astype(jnp.float32)
    terms = jnp.where(use_token[:, :, None], picked, mask_vectors.astype(jnp.float32)[:, None, :])
    embedded = lax.optimization_barrier(jnp.sum(terms, axis=0))
    normed = layer_norm(embedded).astype(jnp.bfloat16)
    queries = jnp.dot(normed, w_qkv[0], preferred_element_type=jnp.float32).astype(jnp.bfloat16)
    key_rows = jnp.dot(normed, w_qkv[1], preferred_element_type=jnp.float32).astype(jnp.bfloat16)
    value_rows = jnp.dot(normed, w_qkv[2], preferred_element_type=jnp.float32).astype(jnp.bfloat16)
    queries, key_rows, value_rows = lax.optimization_barrier((queries, key_rows, value_rows))
    query_three = queries.astype(jnp.float32).reshape(FRAMES, HEADS, HEAD_DIM)
    key_three = key_rows.astype(jnp.float32).reshape(FRAMES, HEADS, HEAD_DIM)
    value_three = value_rows.astype(jnp.float32).reshape(FRAMES, HEADS, HEAD_DIM)
    scores = jnp.einsum('qhd,khd->hqk', query_three, key_three) * HEAD_DIM ** (-0.5)
    row_max = lax.optimization_barrier(jnp.max(scores, axis=-1, keepdims=True))
    weights = jnp.exp(scores - row_max)
    weight_sum = lax.optimization_barrier(jnp.sum(weights, axis=-1))
    rounded = lax.optimization_barrier(weights.astype(jnp.bfloat16)).astype(jnp.float32)
    mixture = jnp.einsum('hqk,khd->qhd', rounded, value_three) / weight_sum.T[:, :, None]
    attended = mixture.reshape(FRAMES, D).astype(jnp.bfloat16)
    after_attn = embedded + jnp.dot(attended, w_out, preferred_element_type=jnp.float32)
    normed_two = layer_norm(after_attn).astype(jnp.bfloat16)
    gate_linear = jnp.dot(normed_two, w_expand, preferred_element_type=jnp.float32)
    gated = (gate_linear[:, :D] * jax.nn.sigmoid(gate_linear[:, D:])).astype(jnp.bfloat16)
    gated = lax.optimization_barrier(gated)
    half_width = KERNEL // 2
    padded = jnp.pad(gated.astype(jnp.float32), ((half_width, half_width), (0, 0)))
    conv = jnp.zeros((FRAMES, D), jnp.float32)
    for tap_index in range(KERNEL):
        conv = conv + padded[tap_index:tap_index + FRAMES] * w_depth[tap_index].astype(jnp.float32)
    activated = (conv * jax.nn.sigmoid(conv)).astype(jnp.bfloat16)
    after_conv = after_attn + jnp.dot(activated, w_project, preferred_element_type=jnp.float32)
    final_norm = layer_norm(after_conv).astype(jnp.bfloat16)
    return jax.vmap(lambda head_one: jnp.dot(final_norm, head_one, preferred_element_type=jnp.float32))(level_heads).astype(jnp.bfloat16)

def reference(token_ids, decoded_mask, levels_done, code_tables, mask_vectors, w_qkv, w_out, w_expand, w_depth, w_project, level_heads):

    def one_clip(clip_parts):
        return clip_step(clip_parts[0], clip_parts[1], clip_parts[2], code_tables, mask_vectors, w_qkv, w_out, w_expand, w_depth, w_project, level_heads)
    return lax.map(one_clip, (token_ids, decoded_mask, levels_done))
```

```python
import functools

import jax
import jax.numpy as jnp
from jax import lax
from jax.experimental import pallas as pl
from jax.experimental.pallas import tpu as pltpu
from jax.sharding import PartitionSpec as P

HEADS = 16
LOG2E = 1.4426950408889634
BF16 = jnp.bfloat16
F32 = jnp.float32
ANY = pl.BlockSpec(memory_space=pl.ANY)
WIDE = pltpu.CompilerParams(vmem_limit_bytes=60 * 2**20)


def layer_norm(values):
    centered = values - jnp.mean(values, axis=-1, keepdims=True)
    variance = jnp.mean(centered * centered, axis=-1, keepdims=True)
    return centered * lax.rsqrt(variance + 1e-05)


def dot(left, right):
    return jnp.dot(left, right, preferred_element_type=F32)


def dot_t(left, right):
    return lax.dot_general(left, right, (((1,), (1,)), ((), ())), preferred_element_type=F32)


def swap(value, bit):
    devices = lax.axis_size("dp")
    return lax.ppermute(value, "dp", [(i, i ^ bit) for i in range(devices)])


def from_outer(value, back):
    devices = lax.axis_size("dp")
    outer = devices // 4
    return lax.ppermute(
        value, "dp", [(i, ((i // 4 + back) % outer) * 4 + i % 4) for i in range(devices)]
    )


def from_level(value, back):
    groups = lax.axis_size("level")
    return lax.ppermute(value, "level", [(i, (i + back) % groups) for i in range(groups)])


def gather_pieces(shard):
    outer = lax.axis_size("dp") // 4
    near = jnp.stack([shard] + [from_outer(shard, back) for back in range(1, outer)])
    far = swap(near, 2)
    crossed = swap(jnp.stack([near, far]), 1)
    return near, far, crossed


def piece_owner(back, pair, core):
    index, outer = lax.axis_index("dp"), lax.axis_size("dp") // 4
    source = lax.rem(index // 4 + outer - back, outer)
    low = lax.rem(index, 4)
    low = jnp.where(pair, 3 - low, low) if pair == core else jnp.where(pair, lax.rem(low + 2, 4), low + 1 - 2 * lax.rem(low, 2))
    return source * 4 + low


def embed_kernel(
    others, outer, rows_here, scale,
    ids_ref, mask_ref, table_ref, *refs,
):
    halves = refs[: 2 * others]
    near_ref, far_ref, crossed_ref = refs[2 * others : 2 * others + 3]
    embedded_ref, queries_ref, keys_ref, values_ref = refs[2 * others + 3 : 2 * others + 7]
    tables, weights, table_sems, weight_sems = refs[2 * others + 7 :]
    step = pl.program_id(0)
    codes = table_ref.shape[0]
    half = codes // 2
    core = lax.rem(lax.axis_index("dp"), 2)

    table_copies = [pltpu.make_async_copy(table_ref, tables.at[pl.ds(0, codes)], table_sems.at[0])]
    for back in range(others):
        base = (back + 1) * codes
        for side in range(2):
            place = base + (core if side == 0 else 1 - core) * half
            table_copies.append(
                pltpu.make_async_copy(
                    halves[2 * back + side],
                    tables.at[pl.ds(place, half)],
                    table_sems.at[1 + 2 * back + side],
                )
            )
    weight_copies = []
    for back in range(outer):
        for pair in range(2):
            for other_core in range(2):
                row = piece_owner(back, pair, other_core) * rows_here
                source = (
                    crossed_ref.at[pair, back] if other_core else (far_ref if pair else near_ref).at[back]
                )
                weight_copies.append(
                    pltpu.make_async_copy(
                        source,
                        weights.at[:, pl.ds(row, rows_here), :],
                        weight_sems.at[len(weight_copies)],
                    )
                )

    @pl.when(step == 0)
    def _():
        for copy in table_copies + weight_copies:
            copy.start()
        for copy in table_copies:
            copy.wait()

    frames = ids_ref.shape[0]
    code_row = lax.broadcasted_iota(jnp.int32, (frames, codes), 1)
    total = None
    for level in range(others + 1):
        ids = ids_ref[:, level : level + 1]
        onehot = jnp.where(ids == code_row, 1.0, 0.0).astype(BF16)
        term = dot(onehot, tables[level * codes : (level + 1) * codes, :])
        fill = mask_ref[level : level + 1, :].astype(F32)
        term = term + jnp.where(ids < 0, fill, 0.0)
        total = term if total is None else total + term
    embedded_ref[...] = total
    normed = layer_norm(total).astype(BF16)

    @pl.when(step == 0)
    def _():
        for copy in weight_copies:
            copy.wait()

    queries_ref[...] = (dot(normed, weights[0]) * scale).astype(BF16)
    keys_ref[...] = dot(normed, weights[1]).astype(BF16)
    values_ref[...] = dot(normed, weights[2]).astype(BF16)


def embed_and_project(ids, masks, table, halves, pieces, scale):
    frames, levels = ids.shape
    codes, width = table.shape
    near, far, crossed = pieces
    outer, three, rows_here, columns = near.shape
    tile = frames // 6
    others = levels - 1
    row_block = lambda i: (i, 0)
    kernel = functools.partial(embed_kernel, others, outer, rows_here, scale)
    flops = 2 * frames * width * (levels * codes + 3 * columns)
    return pl.pallas_call(
        kernel,
        grid=(frames // tile,),
        in_specs=[
            pl.BlockSpec((tile, levels), row_block),
            pl.BlockSpec(masks.shape, lambda i: (0, 0)),
        ]
        + [ANY] * (4 + 2 * others),
        out_specs=[pl.BlockSpec((tile, width), row_block)]
        + [pl.BlockSpec((tile, columns), row_block)] * 3,
        out_shape=[jax.ShapeDtypeStruct((frames, width), F32)]
        + [jax.ShapeDtypeStruct((frames, columns), BF16)] * 3,
        scratch_shapes=[
            pltpu.VMEM((levels * codes, width), BF16),
            pltpu.VMEM((three, width, columns), BF16),
            pltpu.SemaphoreType.DMA((1 + 2 * others,)),
            pltpu.SemaphoreType.DMA((4 * outer,)),
        ],
        compiler_params=WIDE,
        cost_estimate=pl.CostEstimate(flops=flops, bytes_accessed=20 * 2**20, transcendentals=0),
        name="embed_project",
    )(ids, masks, table, *halves, near, far, crossed)


def attention_kernel(head_dim, queries_ref, keys_ref, values_ref, out_ref):
    queries, keys, values = queries_ref[...], keys_ref[...], values_ref[...]
    lane = lax.broadcasted_iota(jnp.int32, (1, 2 * head_dim), 1)
    first = lane < head_dim
    owns = (first, lane >= head_dim)
    scores = [dot_t(jnp.where(own, queries, jnp.zeros_like(queries)), keys) for own in owns]
    sums = []
    for own, score in zip(owns, scores):
        blocks = [score[:, at : at + 128] for at in range(0, score.shape[1], 128)]
        top = functools.reduce(jnp.maximum, blocks)
        top = jnp.max(top, axis=1, keepdims=True)
        weights = jnp.exp2(score - top).astype(BF16)
        sums.append(dot(weights, jnp.where(own, values, jnp.ones_like(values))))
    mixed = jnp.where(first, sums[0], sums[1])
    total = pltpu.roll(jnp.where(first, sums[1], sums[0]), head_dim, 1)
    out_ref[...] = (mixed / total).astype(BF16)


def attend(queries, keys, values, pair, head_dim):
    frames = queries.shape[0]
    width = 2 * head_dim
    tile = frames // 2
    return pl.pallas_call(
        functools.partial(attention_kernel, head_dim),
        grid=(frames // tile,),
        in_specs=[
            pl.BlockSpec((tile, width), lambda i: (i, pair)),
            pl.BlockSpec((frames, width), lambda i: (0, pair)),
            pl.BlockSpec((frames, width), lambda i: (0, pair)),
        ],
        out_specs=pl.BlockSpec((tile, width), lambda i: (i, 0)),
        out_shape=jax.ShapeDtypeStruct((frames, width), BF16),
        compiler_params=WIDE,
        cost_estimate=pl.CostEstimate(
            flops=16 * frames * frames * width, bytes_accessed=2**21, transcendentals=2 * frames * frames
        ),
        name="attend",
    )(queries, keys, values)


def finish_kernel(
    tiles, parts, width,
    embedded_ref, *refs,
):
    att_refs = refs[:parts]
    packed_ref, depth_ref, head_ref, out_ref = refs[parts : parts + 4]
    attended, residual, gated, packed, head, sems = refs[parts + 4 :]
    step = pl.program_id(0)
    tile = embedded_ref.shape[0]
    taps = depth_ref.shape[0]
    reach = taps // 2
    edge = 8
    copies = [
        pltpu.make_async_copy(packed_ref, packed, sems.at[0]),
        pltpu.make_async_copy(head_ref, head, sems.at[1]),
    ]

    @pl.when(step == 0)
    def _():
        for copy in copies:
            copy.start()
        gated[...] = jnp.zeros_like(gated)
        residual[...] = jnp.zeros_like(residual)
        for copy in copies:
            copy.wait()

    before = gated[edge + tile - edge : edge + tile, :]
    previous = gated[edge + tile :, :]
    gated[0:edge, :] = before
    gated[edge : edge + tile, :] = previous
    last_residual = residual[...]

    piece = att_refs[0].shape[1]
    for part, ref in enumerate(att_refs):
        attended[:, part * piece : (part + 1) * piece] = ref[...]
    after = embedded_ref[...] + dot_t(attended[...], packed[:, :width])
    residual[...] = after
    linear = dot(layer_norm(after).astype(BF16), packed[:, width : 3 * width])
    fresh = (linear[:, :width] * jax.nn.sigmoid(linear[:, width:])).astype(BF16).astype(F32)
    fresh = jnp.where(step < tiles, fresh, 0.0)
    gated[edge + tile :, :] = fresh

    conv = None
    for tap in range(taps):
        start = edge - reach + tap
        term = gated[start : start + tile, :] * depth_ref[tap : tap + 1, :].astype(F32)
        conv = term if conv is None else conv + term
    activated = (conv * jax.nn.sigmoid(conv)).astype(BF16)
    after_conv = last_residual + dot(activated, packed[:, 3 * width :])
    out_ref[...] = dot(layer_norm(after_conv).astype(BF16), head[...]).astype(BF16)


def finish(embedded, attended, packed, w_depth, head):
    frames, width = embedded.shape
    codes = head.shape[1]
    tile = frames // 6
    tiles = frames // tile
    parts = len(attended)
    front = lambda i: (jnp.minimum(i, tiles - 1), 0)
    back = lambda i: (jnp.maximum(i - 1, 0), 0)
    flops = 2 * frames * width * (4 * width + codes)
    return pl.pallas_call(
        functools.partial(finish_kernel, tiles, parts, width),
        grid=(tiles + 1,),
        in_specs=[pl.BlockSpec((tile, width), front)]
        + [pl.BlockSpec((tile, part.shape[1]), front) for part in attended]
        + [ANY, pl.BlockSpec(w_depth.shape, lambda i: (0, 0)), ANY],
        out_specs=pl.BlockSpec((tile, codes), back),
        out_shape=jax.ShapeDtypeStruct((frames, codes), BF16),
        scratch_shapes=[
            pltpu.VMEM((tile, width), BF16),
            pltpu.VMEM((tile, width), F32),
            pltpu.VMEM((8 + 2 * tile, width), F32),
            pltpu.VMEM(packed.shape, BF16),
            pltpu.VMEM(head.shape, BF16),
            pltpu.SemaphoreType.DMA((2,)),
        ],
        compiler_params=WIDE,
        cost_estimate=pl.CostEstimate(flops=flops, bytes_accessed=20 * 2**20, transcendentals=0),
        name="finish",
    )(embedded, *attended, packed, w_depth, head)


def body(
    token_ids,
    decoded_mask,
    levels_done,
    code_tables,
    mask_vectors,
    w_qkv,
    w_out,
    w_expand,
    w_depth,
    w_project,
    level_heads,
):
    groups = lax.axis_size("level")
    level_index = lax.axis_index("level")
    table = code_tables[0]
    codes, width = table.shape
    head_dim = width // HEADS
    half = codes // 2
    core = lax.rem(lax.axis_index("dp"), 2)

    own_out = w_out.T
    columns = own_out.shape[1]
    small = jnp.concatenate([own_out, mask_vectors.reshape(-1, columns)], axis=0)
    smalls = [small] + [from_level(small, back) for back in range(1, groups)]
    rows = own_out.shape[0]
    packed = jnp.concatenate([s[:rows] for s in smalls] + [w_expand, w_project], axis=1)
    packed = lax.all_gather(packed, "dp", axis=0, tiled=True)
    masks = jnp.concatenate([s[rows:].reshape(1, width) for s in smalls], axis=0)

    done = levels_done[0]
    use_token = (level_index < done) | ((level_index == done) & (decoded_mask[0, 0] == 1))
    own_ids = jnp.where(use_token, token_ids[0, 0], -1)
    ids = jnp.stack([own_ids] + [from_level(own_ids, back) for back in range(1, groups)], axis=1)

    mine = lax.dynamic_slice_in_dim(table, core * half, half, 0)
    halves = []
    for back in range(1, groups):
        landed = from_level(mine, back)
        halves += [landed, swap(landed, 1)]
    pieces = gather_pieces(w_qkv)

    scale = head_dim ** (-0.5) * LOG2E
    embedded, queries, keys, values = embed_and_project(ids, masks, table, halves, pieces, scale)

    own_parts, far_parts = [], [[] for _ in range(groups - 1)]
    for pair in range(columns // (2 * head_dim)):
        part = attend(queries, keys, values, pair, head_dim)
        own_parts.append(part)
        for back in range(1, groups):
            far_parts[back - 1].append(from_level(part, back))
    attended = own_parts + [part for parts in far_parts for part in parts]
    logits = finish(embedded, attended, packed, w_depth, level_heads[0])
    return logits[None, None]


def solution(mesh):
    return jax.shard_map(
        body,
        mesh=mesh,
        in_specs=(
            P("dp", "level", None),
            P("dp", "level", None),
            P("dp"),
            P("level", None, None),
            P("level", None),
            P(None, "dp", "level"),
            P("level", "dp"),
            P("dp", None),
            P(),
            P("dp", None),
            P("level", None, None),
        ),
        out_specs=P("dp", "level", None, None),
        check_vma=False,
    )
```

```python
import functools

import jax
import jax.numpy as jnp
from jax import lax
from jax.experimental import pallas as pl
from jax.experimental.pallas import tpu as pltpu
from jax.sharding import PartitionSpec as P


HEADS = 16
LOG2E = 1.4426950408889634
BF16 = jnp.bfloat16
F32 = jnp.float32
ANY = pl.BlockSpec(memory_space=pl.ANY)
QUARTERS = 4
CHUNKS = 2
WIDE = pltpu.CompilerParams(vmem_limit_bytes=60 * 2**20)


def layer_norm(values):
    centered = values - jnp.mean(values, axis=-1, keepdims=True)
    variance = jnp.mean(centered * centered, axis=-1, keepdims=True)
    return centered * lax.rsqrt(variance + 1e-05)


def dot(left, right):
    return jnp.dot(left, right, preferred_element_type=F32)


def dot_t(left, right):
    return lax.dot_general(left, right, (((1,), (1,)), ((), ())), preferred_element_type=F32)


def swap(value, bit):
    devices = lax.axis_size("dp")
    return lax.ppermute(value, "dp", [(i, i ^ bit) for i in range(devices)])


def from_outer(value, back):
    devices = lax.axis_size("dp")
    outer = devices // 4
    return lax.ppermute(
        value, "dp", [(i, ((i // 4 + back) % outer) * 4 + i % 4) for i in range(devices)]
    )


def from_level(value, back):
    groups = lax.axis_size("level")
    return lax.ppermute(value, "level", [(i, (i + back) % groups) for i in range(groups)])


def gather_pieces(shard):
    outer = lax.axis_size("dp") // 4
    near = jnp.stack([shard] + [from_outer(shard, back) for back in range(1, outer)])
    far = swap(near, 2)
    crossed = swap(jnp.stack([near, far]), 1)
    return near, far, crossed


def piece_owner(back, pair, core):
    index, outer = lax.axis_index("dp"), lax.axis_size("dp") // 4
    source = lax.rem(index // 4 + outer - back, outer)
    own_pair, own_core = lax.rem(index // 2, 2), lax.rem(index, 2)
    return source * 4 + (1 - own_pair if pair else own_pair) * 2 + (1 - own_core if core else own_core)


def own_term_kernel(ids_ref, mask_ref, table_ref, out_ref):
    code_row = lax.broadcasted_iota(jnp.int32, (1, table_ref.shape[0]), 1)
    ids = ids_ref[:, :1]
    onehot = jnp.where(ids == code_row, 1.0, 0.0).astype(BF16)
    fill = jnp.where(ids < 0, mask_ref[...].astype(F32), 0.0)
    out_ref[...] = (dot(onehot, table_ref[...]) + fill).astype(BF16)


def own_term(ids, mask, table, tile):
    frames = ids.shape[0]
    codes, width = table.shape
    row_block = lambda i: (i, 0)
    return pl.pallas_call(
        own_term_kernel,
        grid=(frames // tile,),
        in_specs=[
            pl.BlockSpec((tile, 1), row_block),
            pl.BlockSpec((1, width), lambda i: (0, 0)),
            pl.BlockSpec((codes, width), lambda i: (0, 0)),
        ],
        out_specs=pl.BlockSpec((tile, width), row_block),
        out_shape=jax.ShapeDtypeStruct((frames, width), BF16),
        compiler_params=WIDE,
        cost_estimate=pl.CostEstimate(
            flops=2 * frames * codes * width, bytes_accessed=2**22, transcendentals=0
        ),
        name="own_term",
    )(ids, mask, table)


def embed_kernel(others, ids_ref, mask_ref, own_ref, *refs):
    halves = refs[: 2 * others]
    embedded_ref, normed_ref, tables, sems = refs[2 * others :]
    step = pl.program_id(0)
    half = halves[0].shape[0]
    codes = 2 * half
    core = lax.rem(lax.axis_index("dp"), 2)
    copies = []
    for index, source in enumerate(halves):
        base, side = (index // 2) * codes, index % 2
        place = base + (core if side == 0 else 1 - core) * half
        copies.append(
            pltpu.make_async_copy(source, tables.at[pl.ds(place, half)], sems.at[index])
        )

    @pl.when(step == 0)
    def _():
        for copy in copies:
            copy.start()
        for copy in copies:
            copy.wait()

    code_row = lax.broadcasted_iota(jnp.int32, (1, codes), 1)
    part = ids_ref.shape[0] // 2
    totals = []
    for sub in range(2):
        rows = slice(sub * part, (sub + 1) * part)
        total = own_ref[rows, :].astype(F32)
        for level in range(others):
            ids = ids_ref[rows, level : level + 1]
            onehot = jnp.where(ids == code_row, 1.0, 0.0).astype(BF16)
            total = total + dot(onehot, tables[level * codes : (level + 1) * codes, :])
            fill = mask_ref[level : level + 1, :].astype(F32)
            total = total + jnp.where(ids < 0, fill, 0.0)
        totals.append(total)
    for sub in range(2):
        rows = slice(sub * part, (sub + 1) * part)
        embedded_ref[rows, :] = totals[sub]
        normed_ref[rows, :] = layer_norm(totals[sub]).astype(BF16)


def embed(ids, masks, own, halves, tile):
    frames, others = ids.shape
    half, width = halves[0].shape
    row_block = lambda i: (i, 0)
    return pl.pallas_call(
        functools.partial(embed_kernel, others),
        grid=(frames // tile,),
        in_specs=[
            pl.BlockSpec((tile, others), row_block),
            pl.BlockSpec(masks.shape, lambda i: (0, 0)),
            pl.BlockSpec((tile, width), row_block),
        ]
        + [ANY] * (2 * others),
        out_specs=[pl.BlockSpec((tile, width), row_block)] * 2,
        out_shape=[
            jax.ShapeDtypeStruct((frames, width), F32),
            jax.ShapeDtypeStruct((frames, width), BF16),
        ],
        scratch_shapes=[
            pltpu.VMEM((2 * others * half, width), BF16),
            pltpu.SemaphoreType.DMA((2 * others,)),
        ],
        compiler_params=WIDE,
        cost_estimate=pl.CostEstimate(
            flops=4 * others * frames * half * width, bytes_accessed=12 * 2**20, transcendentals=0
        ),
        name="embed",
    )(ids, masks, own, *halves)


def project_kernel(chunks, outer, scale, normed_ref, *refs):
    pieces = refs[: 3 * chunks]
    queries_ref, keys_ref, values_ref, weights, sems = refs[3 * chunks :]
    rows_here, columns = pieces[0].shape[2:]
    copies = []
    for chunk in range(chunks):
        near_ref, far_ref, crossed_ref = pieces[3 * chunk : 3 * chunk + 3]
        for back in range(outer):
            for pair in range(2):
                for core in range(2):
                    row = piece_owner(back, pair, core) * rows_here
                    source = crossed_ref.at[pair, back] if core else (far_ref if pair else near_ref).at[back]
                    target = weights.at[chunk, :, pl.ds(row, rows_here), :]
                    copies.append(pltpu.make_async_copy(source, target, sems.at[len(copies)]))

    @pl.when(pl.program_id(0) == 0)
    def _():
        for copy in copies:
            copy.start()
        for copy in copies:
            copy.wait()

    normed = normed_ref[...]
    for chunk in range(chunks):
        at = slice(chunk * columns, (chunk + 1) * columns)
        queries_ref[:, at] = (dot(normed, weights[chunk, 0]) * scale).astype(BF16)
        keys_ref[:, at] = dot(normed, weights[chunk, 1]).astype(BF16)
        values_ref[:, at] = dot(normed, weights[chunk, 2]).astype(BF16)


def project(normed, pieces, scale, tile):
    frames, width = normed.shape
    chunks = len(pieces)
    outer, three, _, columns = pieces[0][0].shape
    row_block = lambda i: (i, 0)
    return pl.pallas_call(
        functools.partial(project_kernel, chunks, outer, scale),
        grid=(frames // tile,),
        in_specs=[pl.BlockSpec((tile, width), row_block)] + [ANY] * (3 * chunks),
        out_specs=[pl.BlockSpec((tile, chunks * columns), row_block)] * 3,
        out_shape=[jax.ShapeDtypeStruct((frames, chunks * columns), BF16)] * 3,
        scratch_shapes=[
            pltpu.VMEM((chunks, three, width, columns), BF16),
            pltpu.SemaphoreType.DMA((4 * outer * chunks,)),
        ],
        compiler_params=WIDE,
        cost_estimate=pl.CostEstimate(
            flops=2 * frames * width * three * columns * chunks, bytes_accessed=12 * 2**20, transcendentals=0
        ),
        name="project",
    )(normed, *[piece for chunk in pieces for piece in chunk])


def attention_kernel(head_dim, queries_ref, keys_ref, values_ref, out_ref):
    queries, keys, values = queries_ref[...], keys_ref[...], values_ref[...]
    lane = lax.broadcasted_iota(jnp.int32, (1, 2 * head_dim), 1)
    first = lane < head_dim
    owns = (first, lane >= head_dim)
    scores = [dot_t(jnp.where(own, queries, jnp.zeros_like(queries)), keys) for own in owns]
    sums = []
    for own, score in zip(owns, scores):
        blocks = [score[:, at : at + 128] for at in range(0, score.shape[1], 128)]
        top = functools.reduce(jnp.maximum, blocks)
        top = jnp.max(top, axis=1, keepdims=True)
        weights = jnp.exp2(score - top).astype(BF16)
        sums.append(dot(weights, jnp.where(own, values, jnp.ones_like(values))))
    mixed = jnp.where(first, sums[0], sums[1])
    total = pltpu.roll(jnp.where(first, sums[1], sums[0]), head_dim, 1)
    out_ref[...] = (mixed / total).astype(BF16)


def attend(queries, keys, values, quarter, tile, head_dim):
    frames, columns = queries.shape
    width = 2 * head_dim
    return pl.pallas_call(
        functools.partial(attention_kernel, head_dim),
        grid=(columns // width,),
        in_specs=[
            pl.BlockSpec((tile, width), lambda p: (quarter, p)),
            pl.BlockSpec((frames, width), lambda p: (0, p)),
            pl.BlockSpec((frames, width), lambda p: (0, p)),
        ],
        out_specs=pl.BlockSpec((tile, width), lambda p: (0, p)),
        out_shape=jax.ShapeDtypeStruct((tile, columns), BF16),
        compiler_params=WIDE,
        cost_estimate=pl.CostEstimate(
            flops=16 * tile * frames * columns, bytes_accessed=2**22, transcendentals=0
        ),
        name="attend",
    )(queries, keys, values)


def gate_kernel(quarters, groups, width, embedded_ref, *refs):
    att_refs = refs[: quarters * groups]
    packed_ref, after_ref, gated_ref, attended, packed, sems = refs[quarters * groups :]
    step = pl.program_id(0)
    copies = [
        pltpu.make_async_copy(packed_ref.at[:, pl.ds(0, width)], packed.at[:, pl.ds(0, width)], sems.at[0]),
        pltpu.make_async_copy(
            packed_ref.at[:, pl.ds(width, 2 * width)], packed.at[:, pl.ds(width, 2 * width)], sems.at[1]
        ),
    ]

    @pl.when(step == 0)
    def _():
        for copy in copies:
            copy.start()

    piece = att_refs[0].shape[1]
    for quarter in range(quarters):

        @pl.when(step == quarter)
        def _():
            for group in range(groups):
                attended[:, group * piece : (group + 1) * piece] = att_refs[quarter * groups + group][...]

    @pl.when(step == 0)
    def _():
        for copy in copies:
            copy.wait()

    part = embedded_ref.shape[0] // 2
    rows = [slice(sub * part, (sub + 1) * part) for sub in range(2)]
    afters = [embedded_ref[r, :] + dot_t(attended[r, :], packed[:, :width]) for r in rows]
    linears = []
    for r, after in zip(rows, afters):
        after_ref[r, :] = after
        linears.append(dot(layer_norm(after).astype(BF16), packed[:, width:]))
    for r, linear in zip(rows, linears):
        gated_ref[r, :] = (linear[:, :width] * jax.nn.sigmoid(linear[:, width:])).astype(BF16)


def gate(embedded, attended, packed, first, tile):
    width = embedded.shape[1]
    quarters, groups = len(attended), len(attended[0])
    flat = [part for parts in attended for part in parts]
    rows = quarters * tile
    return pl.pallas_call(
        functools.partial(gate_kernel, quarters, groups, width),
        grid=(quarters,),
        in_specs=[pl.BlockSpec((tile, width), lambda i: (first + i, 0))]
        + [pl.BlockSpec(part.shape, lambda i: (0, 0)) for part in flat]
        + [ANY],
        out_specs=[pl.BlockSpec((tile, width), lambda i: (i, 0))] * 2,
        out_shape=[
            jax.ShapeDtypeStruct((rows, width), F32),
            jax.ShapeDtypeStruct((rows, width), BF16),
        ],
        scratch_shapes=[
            pltpu.VMEM((tile, width), BF16),
            pltpu.VMEM((width, 3 * width), BF16),
            pltpu.SemaphoreType.DMA((2,)),
        ],
        compiler_params=WIDE,
        cost_estimate=pl.CostEstimate(
            flops=6 * rows * width * width, bytes_accessed=12 * 2**20, transcendentals=0
        ),
        name="gate",
    )(embedded, *flat, packed)


def finish_kernel(tiles, halves, *refs):
    gated_refs, after_refs = refs[: 3 * halves], refs[3 * halves : 4 * halves]
    packed_ref, depth_ref, head_ref, out_ref, window, residual, project, head, sems = refs[4 * halves :]
    step = pl.program_id(0)
    tile, width = residual.shape
    taps = depth_ref.shape[0]
    edge = 8
    copies = [
        pltpu.make_async_copy(packed_ref.at[:, pl.ds(3 * width, width)], project, sems.at[0]),
        pltpu.make_async_copy(head_ref, head, sems.at[1]),
    ]

    @pl.when(step == 0)
    def _():
        for copy in copies:
            copy.start()

    per_half = tiles // halves
    for half in range(halves):
        before_ref, here_ref, next_ref = gated_refs[3 * half : 3 * half + 3]

        @pl.when(step // per_half == half)
        def _():
            window[edge : edge + tile, :] = here_ref[...].astype(F32)
            residual[...] = after_refs[half][...]

        @pl.when((step > 0) & ((step - 1) // per_half == half))
        def _():
            window[:edge, :] = before_ref[...].astype(F32)[-edge:, :]

        @pl.when((step < tiles - 1) & ((step + 1) // per_half == half))
        def _():
            window[edge + tile :, :] = next_ref[...].astype(F32)[:edge, :]

    @pl.when(step == 0)
    def _():
        window[:edge, :] = jnp.zeros((edge, width), F32)

    @pl.when(step == tiles - 1)
    def _():
        window[edge + tile :, :] = jnp.zeros((edge, width), F32)

    @pl.when(step == 0)
    def _():
        for copy in copies:
            copy.wait()

    part = tile // 2
    rows = [slice(sub * part, (sub + 1) * part) for sub in range(2)]
    sums = []
    for r in rows:
        conv = None
        for tap in range(taps):
            start = r.start + edge - taps // 2 + tap
            term = window[start : start + part, :] * depth_ref[tap : tap + 1, :].astype(F32)
            conv = term if conv is None else conv + term
        activated = (conv * jax.nn.sigmoid(conv)).astype(BF16)
        sums.append(residual[r, :] + dot(activated, project[...]))
    for r, after_conv in zip(rows, sums):
        out_ref[r, :] = dot(layer_norm(after_conv).astype(BF16), head[...]).astype(BF16)


def finish(gated, after, packed, w_depth, head, tile):
    halves = len(gated)
    half_rows, width = gated[0].shape
    codes = head.shape[1]
    frames = halves * half_rows
    tiles = frames // tile
    per_half = half_rows // tile
    strip = 16
    per_tile = tile // strip

    def clip(index, half):
        return jnp.clip(index - half * per_half, 0, per_half - 1)

    specs = []
    for half in range(halves):
        specs += [
            pl.BlockSpec((strip, width), lambda i, half=half: (clip(i - 1, half) * per_tile + per_tile - 1, 0)),
            pl.BlockSpec((tile, width), lambda i, half=half: (clip(i, half), 0)),
            pl.BlockSpec((strip, width), lambda i, half=half: (clip(i + 1, half) * per_tile, 0)),
        ]
    for half in range(halves):
        specs.append(pl.BlockSpec((tile, width), lambda i, half=half: (clip(i, half), 0)))
    return pl.pallas_call(
        functools.partial(finish_kernel, tiles, halves),
        grid=(tiles,),
        in_specs=specs + [ANY, pl.BlockSpec(w_depth.shape, lambda i: (0, 0)), ANY],
        out_specs=pl.BlockSpec((tile, codes), lambda i: (i, 0)),
        out_shape=jax.ShapeDtypeStruct((frames, codes), BF16),
        scratch_shapes=[
            pltpu.VMEM((tile + 16, width), F32),
            pltpu.VMEM((tile, width), F32),
            pltpu.VMEM((width, width), BF16),
            pltpu.VMEM(head.shape, BF16),
            pltpu.SemaphoreType.DMA((2,)),
        ],
        compiler_params=WIDE,
        cost_estimate=pl.CostEstimate(
            flops=2 * frames * width * (width + codes), bytes_accessed=20 * 2**20, transcendentals=0
        ),
        name="finish",
    )(*[g for half in gated for g in (half, half, half)], *after, packed, w_depth, head)


def body(
    token_ids,
    decoded_mask,
    levels_done,
    code_tables,
    mask_vectors,
    w_qkv,
    w_out,
    w_expand,
    w_depth,
    w_project,
    level_heads,
):
    return step(
        token_ids[0, 0], decoded_mask[0, 0], levels_done[0], code_tables[0], mask_vectors,
        w_qkv, w_out, w_expand, w_depth, w_project, level_heads[0],
    )[None, None]


def step(
    token_ids, decoded_mask, done, table, own_mask, w_qkv, w_out, w_expand, w_depth, w_project, head,
):
    groups = lax.axis_size("level")
    level_index = lax.axis_index("level")
    frames = token_ids.shape[0]
    codes, width = table.shape
    head_dim = width // HEADS
    half = codes // 2
    core = lax.rem(lax.axis_index("dp"), 2)
    backs = range(1, groups)

    own_out = w_out.T
    rows, columns = own_out.shape
    small = jnp.concatenate([own_out, own_mask.reshape(-1, columns)], axis=0)
    smalls = [small] + [from_level(small, back) for back in backs]
    packed = jnp.concatenate([s[:rows] for s in smalls] + [w_expand, w_project], axis=1)
    packed = lax.all_gather(packed, "dp", axis=0, tiled=True)

    use_token = (level_index < done) | ((level_index == done) & (decoded_mask == 1))
    own_ids = jnp.where(use_token, token_ids, -1)
    ids = jnp.stack([from_level(own_ids, back) for back in backs], axis=1)
    masks = jnp.concatenate([s[rows:].reshape(1, width) for s in smalls[1:]], axis=0)

    mine = lax.dynamic_slice_in_dim(table, core * half, half, 0)
    halves = []
    for back in backs:
        landed = from_level(mine, back)
        halves += [landed, swap(landed, 1)]
    pieces = []
    chunk = columns // CHUNKS
    for at in range(CHUNKS):
        pieces.append(gather_pieces(w_qkv[:, :, at * chunk : (at + 1) * chunk]))

    tile = frames // QUARTERS
    own = own_term(own_ids[:, None], own_mask, table, tile)
    embedded, normed = embed(ids, masks, own, halves, tile)
    scale = head_dim ** (-0.5) * LOG2E
    queries, keys, values = project(normed, pieces, scale, tile)

    attended = []
    for quarter in range(QUARTERS):
        part = attend(queries, keys, values, quarter, tile, head_dim)
        attended.append([part] + [from_level(part, back) for back in backs])
    after, gated = [], []
    per_half = QUARTERS // 2
    for part in range(2):
        some = attended[part * per_half : (part + 1) * per_half]
        result = gate(embedded, some, packed, part * per_half, tile)
        after.append(result[0])
        gated.append(result[1])
    return finish(gated, after, packed, w_depth, head, tile)


def solution(mesh):
    return jax.shard_map(
        body,
        mesh=mesh,
        in_specs=(
            P("dp", "level", None),
            P("dp", "level", None),
            P("dp"),
            P("level", None, None),
            P("level", None),
            P(None, "dp", "level"),
            P("level", "dp"),
            P("dp", None),
            P(),
            P("dp", None),
            P("level", None, None),
        ),
        out_specs=P("dp", "level", None, None),
        check_vma=False,
    )
```

```python
import functools

import jax
import jax.numpy as jnp
from jax import lax
from jax.experimental import pallas as pl
from jax.experimental.pallas import tpu as pltpu
from jax.sharding import PartitionSpec as P


HEADS = 16
LOG2E = 1.4426950408889634
BF16 = jnp.bfloat16
F32 = jnp.float32
ANY = pl.BlockSpec(memory_space=pl.ANY)
QUARTERS = 4
CHUNKS = 2
STRIP = 16
SUBS = 3


def grant(mebibytes):
    return pltpu.CompilerParams(vmem_limit_bytes=mebibytes * 2**20)


def layer_norm(values):
    centered = values - jnp.mean(values, axis=-1, keepdims=True)
    variance = jnp.mean(centered * centered, axis=-1, keepdims=True)
    return centered * lax.rsqrt(variance + 1e-05)


def gate_of(values):
    return 0.5 * jnp.tanh(0.5 * values) + 0.5


def dot(left, right):
    return jnp.dot(left, right, preferred_element_type=F32)


def dot_t(left, right):
    return lax.dot_general(left, right, (((1,), (1,)), ((), ())), preferred_element_type=F32)


def swap(value, bit):
    devices = lax.axis_size("dp")
    return lax.ppermute(value, "dp", [(i, i ^ bit) for i in range(devices)])


def from_outer(value, back):
    devices = lax.axis_size("dp")
    outer = devices // 4
    return lax.ppermute(
        value, "dp", [(i, ((i // 4 + back) % outer) * 4 + i % 4) for i in range(devices)]
    )


def from_level(value, back):
    groups = lax.axis_size("level")
    return lax.ppermute(value, "level", [(i, (i + back) % groups) for i in range(groups)])


def gather_pieces(shard):
    outer = lax.axis_size("dp") // 4
    near = [shard] + [from_outer(shard, back) for back in range(1, outer)]
    near = jnp.stack(near)
    far = swap(near, 2)
    return near, far, swap(near, 1), swap(far, 1)


def piece_copies(pieces, place, sems):
    outer, rows_here = pieces[0].shape[0], pieces[0].shape[-2]
    copies = []
    for side, piece in enumerate(pieces):
        for back in range(outer):
            row = piece_owner(back, side % 2, side // 2) * rows_here
            target = place(pl.ds(row, rows_here))
            copies.append(pltpu.make_async_copy(piece.at[back], target, sems.at[len(copies)]))
    return copies


def piece_owner(back, pair, core):
    index, outer = lax.axis_index("dp"), lax.axis_size("dp") // 4
    source = lax.rem(index // 4 + outer - back, outer)
    own_pair, own_core = lax.rem(index // 2, 2), lax.rem(index, 2)
    return source * 4 + (1 - own_pair if pair else own_pair) * 2 + (1 - own_core if core else own_core)


def own_term_kernel(ids_ref, mask_ref, table_ref, out_ref):
    code_row = lax.broadcasted_iota(jnp.int32, (1, table_ref.shape[0]), 1)
    ids = ids_ref[:, :1]
    onehot = jnp.where(ids == code_row, 1.0, 0.0).astype(BF16)
    fill = jnp.where(ids < 0, mask_ref[...].astype(F32), 0.0)
    out_ref[...] = (dot(onehot, table_ref[...]) + fill).astype(BF16)


def own_term(ids, mask, table, tile):
    frames = ids.shape[0]
    codes, width = table.shape
    row_block = lambda i: (i, 0)
    return pl.pallas_call(
        own_term_kernel,
        grid=(frames // tile,),
        in_specs=[
            pl.BlockSpec((tile, 1), row_block),
            pl.BlockSpec((1, width), lambda i: (0, 0)),
            pl.BlockSpec((codes, width), lambda i: (0, 0)),
        ],
        out_specs=pl.BlockSpec((tile, width), row_block),
        out_shape=jax.ShapeDtypeStruct((frames, width), BF16),
        compiler_params=grant(14),
        cost_estimate=pl.CostEstimate(
            flops=2 * frames * codes * width, bytes_accessed=2**22, transcendentals=0
        ),
        name="own_term",
    )(ids, mask, table)


def project_kernel(others, chunks, scale, ids_ref, mask_ref, own_ref, *refs):
    halves, pieces = refs[: 2 * others], refs[2 * others : 2 * others + 4 * chunks]
    embedded_ref, queries_ref, keys_ref, values_ref = refs[2 * others + 4 * chunks :][:4]
    tables, weights, table_sems, weight_sems = refs[2 * others + 4 * chunks + 4 :]
    codes = tables.shape[0] // others
    half = codes // 2
    core = lax.rem(lax.axis_index("dp"), 2)
    copies = []
    for index, source in enumerate(halves):
        base, side = (index // 2) * codes, index % 2
        place = base + (core if side == 0 else 1 - core) * half
        target = tables.at[pl.ds(place, half)]
        copies.append(
            pltpu.make_async_copy(source.at[pl.ds(0, half)], target, table_sems.at[index])
        )
    columns = pieces[0].shape[-1]
    for chunk in range(chunks):
        lanes = pl.ds(chunk * columns, columns)
        copies += piece_copies(
            pieces[4 * chunk : 4 * chunk + 4],
            lambda rows, lanes=lanes: weights.at[:, rows, lanes],
            weight_sems.at[chunk],
        )

    @pl.when(pl.program_id(0) == 0)
    def _():
        for copy in copies:
            copy.start()
        for copy in copies:
            copy.wait()

    code_row = lax.broadcasted_iota(jnp.int32, (1, codes), 1)
    part = ids_ref.shape[0] // 2
    rows = [slice(sub * part, (sub + 1) * part) for sub in range(2)]
    totals = []
    for r in rows:
        total = own_ref[r, :].astype(F32)
        for level in range(others):
            ids = ids_ref[r, level : level + 1]
            onehot = jnp.where(ids == code_row, 1.0, 0.0).astype(BF16)
            total = total + dot(onehot, tables[level * codes : (level + 1) * codes, :])
            fill = mask_ref[level : level + 1, :].astype(F32)
            total = total + jnp.where(ids < 0, fill, 0.0)
        totals.append(total)
    for r, total in zip(rows, totals):
        embedded_ref[r, :] = total
        normed = layer_norm(total).astype(BF16)
        queries_ref[r, :] = (dot(normed, weights[0]) * scale).astype(BF16)
        keys_ref[r, :] = dot(normed, weights[1]).astype(BF16)
        values_ref[r, :] = dot(normed, weights[2]).astype(BF16)


def embed_and_project(ids, masks, own, halves, half, pieces, scale, tile):
    frames, others = ids.shape
    width = own.shape[1]
    chunks = len(pieces)
    outer, three, _, columns = pieces[0][0].shape
    columns *= chunks
    row_block = lambda i: (i, 0)
    return pl.pallas_call(
        functools.partial(project_kernel, others, chunks, scale),
        grid=(frames // tile,),
        in_specs=[
            pl.BlockSpec((tile, others), row_block),
            pl.BlockSpec(masks.shape, lambda i: (0, 0)),
            pl.BlockSpec((tile, width), row_block),
        ]
        + [ANY] * (2 * others + 4 * chunks),
        out_specs=[pl.BlockSpec((tile, width), row_block)]
        + [pl.BlockSpec((tile, columns), row_block)] * 3,
        out_shape=[jax.ShapeDtypeStruct((frames, width), F32)]
        + [jax.ShapeDtypeStruct((frames, columns), BF16)] * 3,
        scratch_shapes=[
            pltpu.VMEM((2 * others * half, width), BF16),
            pltpu.VMEM((three, width, columns), BF16),
            pltpu.SemaphoreType.DMA((2 * others,)),
            pltpu.SemaphoreType.DMA((chunks, 4 * outer)),
        ],
        compiler_params=grant(24 if others == 1 else 44),
        cost_estimate=pl.CostEstimate(
            flops=2 * frames * width * (2 * half * others + three * columns),
            bytes_accessed=20 * 2**20,
            transcendentals=0,
        ),
        name="project",
    )(ids, masks, own, *halves, *[piece for chunk in pieces for piece in chunk])


def attention_kernel(head_dim, queries_ref, keys_ref, values_ref, out_ref):
    queries, keys, values = queries_ref[...], keys_ref[...], values_ref[...]
    lane = lax.broadcasted_iota(jnp.int32, (1, 2 * head_dim), 1)
    first = lane < head_dim
    owns = (first, lane >= head_dim)
    scores = [dot_t(jnp.where(own, queries, jnp.zeros_like(queries)), keys) for own in owns]
    sums = []
    for own, score in zip(owns, scores):
        blocks = [score[:, at : at + 128] for at in range(0, score.shape[1], 128)]
        top = functools.reduce(jnp.maximum, blocks)
        top = jnp.max(top, axis=1, keepdims=True)
        weights = jnp.exp2(score - top).astype(BF16)
        sums.append(dot(weights, jnp.where(own, values, jnp.ones_like(values))))
    mixed = jnp.where(first, sums[0], sums[1])
    total = pltpu.roll(jnp.where(first, sums[1], sums[0]), head_dim, 1)
    out_ref[...] = (mixed / total).astype(BF16)


def attend(queries, keys, values, quarter, tile, head_dim):
    frames, columns = queries.shape
    width = 2 * head_dim
    return pl.pallas_call(
        functools.partial(attention_kernel, head_dim),
        grid=(columns // width,),
        in_specs=[
            pl.BlockSpec((tile, width), lambda p: (quarter, p)),
            pl.BlockSpec((frames, width), lambda p: (0, p)),
            pl.BlockSpec((frames, width), lambda p: (0, p)),
        ],
        out_specs=pl.BlockSpec((tile, width), lambda p: (0, p)),
        out_shape=jax.ShapeDtypeStruct((tile, columns), BF16),
        compiler_params=grant(20),
        cost_estimate=pl.CostEstimate(
            flops=16 * tile * frames * columns, bytes_accessed=2**22, transcendentals=0
        ),
        name="attend",
    )(queries, keys, values)


def gate_kernel(quarters, groups, width, embedded_ref, *refs):
    att_refs = refs[: quarters * groups]
    late = refs[quarters * groups :][:8]
    after_ref, gated_ref, attended, packed, sems = refs[quarters * groups + 8 :]
    step = pl.program_id(0)
    first = piece_copies(late[:4], lambda rows: packed.at[rows, pl.ds(0, 2 * width)], sems.at[0])
    second = piece_copies(
        [ref.at[:, :, pl.ds(0, width)] for ref in late[4:]],
        lambda rows: packed.at[rows, pl.ds(2 * width, width)],
        sems.at[1],
    )
    copies = first + second

    @pl.when(step == 0)
    def _():
        for copy in copies:
            copy.start()

    piece = att_refs[0].shape[1]
    for quarter in range(quarters):

        @pl.when(step == quarter)
        def _():
            for group in range(groups):
                attended[:, group * piece : (group + 1) * piece] = att_refs[quarter * groups + group][...]

    @pl.when(step == 0)
    def _():
        for copy in copies:
            copy.wait()

    part = embedded_ref.shape[0] // 2
    rows = [slice(sub * part, (sub + 1) * part) for sub in range(2)]
    afters = [embedded_ref[r, :] + dot_t(attended[r, :], packed[:, :width]) for r in rows]
    linears = []
    for r, after in zip(rows, afters):
        after_ref[r, :] = after
        linears.append(dot(layer_norm(after).astype(BF16), packed[:, width:]))
    for r, linear in zip(rows, linears):
        gated_ref[r, :] = (linear[:, :width] * gate_of(linear[:, width:])).astype(BF16)


def gate(embedded, attended, late, first, tile):
    width = embedded.shape[1]
    quarters, groups = len(attended), len(attended[0])
    flat = [part for parts in attended for part in parts]
    rows = quarters * tile
    return pl.pallas_call(
        functools.partial(gate_kernel, quarters, groups, width),
        grid=(quarters,),
        in_specs=[pl.BlockSpec((tile, width), lambda i: (first + i, 0))]
        + [pl.BlockSpec(part.shape, lambda i: (0, 0)) for part in flat]
        + [ANY] * len(late),
        out_specs=[pl.BlockSpec((tile, width), lambda i: (i, 0))] * 2,
        out_shape=[
            jax.ShapeDtypeStruct((rows, width), F32),
            jax.ShapeDtypeStruct((rows, width), BF16),
        ],
        scratch_shapes=[
            pltpu.VMEM((tile, width), BF16),
            pltpu.VMEM((width, 3 * width), BF16),
            pltpu.SemaphoreType.DMA((2, 4 * late[0].shape[0])),
        ],
        compiler_params=grant(22),
        cost_estimate=pl.CostEstimate(
            flops=6 * rows * width * width, bytes_accessed=12 * 2**20, transcendentals=0
        ),
        name="gate",
    )(embedded, *flat, *late)


def finish_kernel(tiles, halves, *refs):
    gated_refs, after_refs = refs[: 3 * halves], refs[3 * halves : 4 * halves]
    late = refs[4 * halves :][:4]
    depth_ref, head_ref, out_ref, window, residual, project, head, sems, head_sem = refs[4 * halves + 4 :]
    step = pl.program_id(0)
    tile, width = residual.shape
    taps = depth_ref.shape[0]
    edge = 8
    copies = piece_copies(
        [ref.at[:, :, pl.ds(width, width)] for ref in late], lambda rows: project.at[rows], sems
    )
    copies.append(pltpu.make_async_copy(head_ref, head, head_sem))

    @pl.when(step == 0)
    def _():
        for copy in copies:
            copy.start()

    per_half = tiles // halves
    for half in range(halves):
        before_ref, here_ref, next_ref = gated_refs[3 * half : 3 * half + 3]

        @pl.when(step // per_half == half)
        def _():
            window[edge : edge + tile, :] = here_ref[...].astype(F32)
            residual[...] = after_refs[half][...]

        @pl.when((step > 0) & ((step - 1) // per_half == half))
        def _():
            window[:edge, :] = before_ref[...].astype(F32)[-edge:, :]

        @pl.when((step < tiles - 1) & ((step + 1) // per_half == half))
        def _():
            window[edge + tile :, :] = next_ref[...].astype(F32)[:edge, :]

    @pl.when(step == 0)
    def _():
        window[:edge, :] = jnp.zeros((edge, width), F32)

    @pl.when(step == tiles - 1)
    def _():
        window[edge + tile :, :] = jnp.zeros((edge, width), F32)

    @pl.when(step == 0)
    def _():
        for copy in copies:
            copy.wait()

    part = tile // SUBS

    def activate(first):
        blocks = []
        for at in range(0, width, 128):
            lanes = slice(at, at + 128)
            near = window[first : first + part + 2 * edge, lanes]
            conv = None
            for tap in range(taps):
                start = edge - taps // 2 + tap
                term = near[start : start + part] * depth_ref[tap : tap + 1, lanes].astype(F32)
                conv = term if conv is None else conv + term
            blocks.append((conv * gate_of(conv)).astype(BF16))
        return jnp.concatenate(blocks, axis=1)

    activated = activate(0)
    waiting = None
    for sub in range(SUBS + 1):
        mixed = None
        if sub < SUBS:
            mixed = dot(activated, project[...])
            if sub + 1 < SUBS:
                activated = activate((sub + 1) * part)
        if sub > 0:
            r = slice((sub - 1) * part, sub * part)
            normed = layer_norm(residual[r, :] + waiting).astype(BF16)
            out_ref[r, :] = dot(normed, head[...]).astype(BF16)
        waiting = mixed


def finish(gated, after, late, w_depth, head, tile):
    halves = len(gated)
    half_rows, width = gated[0].shape
    codes = head.shape[1]
    frames = halves * half_rows
    tiles = frames // tile
    per_half = half_rows // tile
    strip = STRIP
    per_tile = tile // strip

    def clip(index, half):
        return jnp.clip(index - half * per_half, 0, per_half - 1)

    specs = []
    for half in range(halves):
        specs += [
            pl.BlockSpec((strip, width), lambda i, half=half: (clip(i - 1, half) * per_tile + per_tile - 1, 0)),
            pl.BlockSpec((tile, width), lambda i, half=half: (clip(i, half), 0)),
            pl.BlockSpec((strip, width), lambda i, half=half: (clip(i + 1, half) * per_tile, 0)),
        ]
    for half in range(halves):
        specs.append(pl.BlockSpec((tile, width), lambda i, half=half: (clip(i, half), 0)))
    return pl.pallas_call(
        functools.partial(finish_kernel, tiles, halves),
        grid=(tiles,),
        in_specs=specs + [ANY] * 4 + [pl.BlockSpec(w_depth.shape, lambda i: (0, 0)), ANY],
        out_specs=pl.BlockSpec((tile, codes), lambda i: (i, 0)),
        out_shape=jax.ShapeDtypeStruct((frames, codes), BF16),
        scratch_shapes=[
            pltpu.VMEM((tile + 16, width), F32),
            pltpu.VMEM((tile, width), F32),
            pltpu.VMEM((width, width), BF16),
            pltpu.VMEM(head.shape, BF16),
            pltpu.SemaphoreType.DMA((4 * late[0].shape[0],)),
            pltpu.SemaphoreType.DMA,
        ],
        compiler_params=grant(22),
        cost_estimate=pl.CostEstimate(
            flops=2 * frames * width * (width + codes), bytes_accessed=20 * 2**20, transcendentals=0
        ),
        name="finish",
    )(*[g for half in gated for g in (half, half, half)], *after, *late, w_depth, head)


def body(
    token_ids,
    decoded_mask,
    levels_done,
    code_tables,
    mask_vectors,
    w_qkv,
    w_out,
    w_expand,
    w_depth,
    w_project,
    level_heads,
):
    return step(
        token_ids[0, 0], decoded_mask[0, 0], levels_done[0], code_tables[0], mask_vectors,
        w_qkv, w_out, w_expand, w_depth, w_project, level_heads[0],
    )[None, None]


def step(
    token_ids, decoded_mask, done, table, own_mask, w_qkv, w_out, w_expand, w_depth, w_project, head,
):
    groups = lax.axis_size("level")
    level_index = lax.axis_index("level")
    frames = token_ids.shape[0]
    codes, width = table.shape
    head_dim = width // HEADS
    half = codes // 2
    core = lax.rem(lax.axis_index("dp"), 2)
    backs = range(1, groups)

    own_out = w_out.T
    columns = own_out.shape[1]
    outs = [own_out] + [from_level(own_out, back) for back in backs]
    late_shards = (
        jnp.concatenate(outs + [w_expand[:, :width]], axis=1),
        jnp.concatenate([w_expand[:, width:], w_project], axis=1),
    )

    use_token = (level_index < done) | ((level_index == done) & (decoded_mask == 1))
    own_ids = jnp.where(use_token, token_ids, -1)
    ids = jnp.stack([from_level(own_ids, back) for back in backs], axis=1)

    mine = lax.dynamic_slice_in_dim(table, core * half, half, 0)
    mine = jnp.concatenate([mine, jnp.broadcast_to(own_mask, (STRIP, width))], axis=0)
    halves, masks = [], []
    for back in backs:
        landed = from_level(mine, back)
        masks.append(landed[half : half + 1])
        halves += [landed, swap(landed, 1)]
    pieces = []
    chunk = columns // CHUNKS if columns % (128 * CHUNKS) == 0 else columns
    for at in range(columns // chunk):
        pieces.append(gather_pieces(w_qkv[:, :, at * chunk : (at + 1) * chunk]))
    late = [gather_pieces(shard) for shard in late_shards]

    tile = frames // QUARTERS
    own = own_term(own_ids[:, None], own_mask, table, tile)
    scale = head_dim ** (-0.5) * LOG2E
    embedded, queries, keys, values = embed_and_project(
        ids, jnp.concatenate(masks), own, halves, half, pieces, scale, tile
    )

    attended = []
    for quarter in range(QUARTERS):
        part = attend(queries, keys, values, quarter, tile, head_dim)
        attended.append([part] + [from_level(part, back) for back in backs])
    after, gated = [], []
    per_half = QUARTERS // 2
    for part in range(2):
        some = attended[part * per_half : (part + 1) * per_half]
        result = gate(embedded, some, late[0] + late[1], part * per_half, tile)
        after.append(result[0])
        gated.append(result[1])
    return finish(gated, after, late[1], w_depth, head, tile)


def solution(mesh):
    return jax.shard_map(
        body,
        mesh=mesh,
        in_specs=(
            P("dp", "level", None),
            P("dp", "level", None),
            P("dp"),
            P("level", None, None),
            P("level", None),
            P(None, "dp", "level"),
            P("level", "dp"),
            P("dp", None),
            P(),
            P("dp", None),
            P("level", None, None),
        ),
        out_specs=P("dp", "level", None, None),
        check_vma=False,
    )
```

```python
import functools

import jax
import jax.numpy as jnp
from jax import lax
from jax.experimental import pallas as pl
from jax.experimental.pallas import tpu as pltpu
from jax.sharding import PartitionSpec as P


HEADS = 16
DP, LEVEL = "dp", "level"
LOG2E = 1.4426950408889634
BF16 = jnp.bfloat16
F32 = jnp.float32
WHOLE = pl.BlockSpec(memory_space=pltpu.VMEM)
QUARTERS = 4
CHUNKS = 2
STRIP = 16
SUBS = 2


def grant(mebibytes):
    return pltpu.CompilerParams(vmem_limit_bytes=mebibytes * 2**20)


def layer_norm(values):
    centered = values - jnp.mean(values, axis=-1, keepdims=True)
    variance = jnp.mean(centered * centered, axis=-1, keepdims=True)
    return centered * lax.rsqrt(variance + 1e-05)


def gate_of(values):
    return 0.5 * jnp.tanh(0.5 * values) + 0.5


def dot(left, right):
    return jnp.dot(left, right, preferred_element_type=F32)


def dot_t(left, right):
    return lax.dot_general(left, right, (((1,), (1,)), ((), ())), preferred_element_type=F32)


def swap(value, bit):
    devices = lax.axis_size(DP)
    return lax.ppermute(value, DP, [(i, i ^ bit) for i in range(devices)])


def from_outer(value, back):
    devices = lax.axis_size(DP)
    outer = devices // 4
    return lax.ppermute(
        value, DP, [(i, ((i // 4 + back) % outer) * 4 + i % 4) for i in range(devices)]
    )


def from_level(value, back):
    groups = lax.axis_size(LEVEL)
    return lax.ppermute(value, LEVEL, [(i, (i + back) % groups) for i in range(groups)])


def gather_outer(shard):
    outer = lax.axis_size(DP) // 4
    return [shard] + [from_outer(shard, back) for back in range(1, outer)]


def gather_chip_pairs(near):
    near = jnp.stack(near)
    far = swap(near, 2)
    return near, far, swap(near, 1), swap(far, 1)


def place_pieces(pieces, target, lanes):
    outer, rows_here = pieces[0].shape[0], pieces[0].shape[-2]
    for side, piece in enumerate(pieces):
        for back in range(outer):
            row = pl.multiple_of(piece_owner(back, side % 2, side // 2) * rows_here, rows_here)
            target[pl.ds(row, rows_here), lanes] = piece[back]


def piece_owner(back, pair, core):
    index, outer = lax.axis_index(DP), lax.axis_size(DP) // 4
    source = lax.rem(index // 4 + outer - back, outer)
    own_pair, own_core = lax.rem(index // 2, 2), lax.rem(index, 2)
    return source * 4 + (1 - own_pair if pair else own_pair) * 2 + (1 - own_core if core else own_core)


def own_term_kernel(ids_ref, mask_ref, table_ref, out_ref):
    code_row = lax.broadcasted_iota(jnp.int32, (1, table_ref.shape[0]), 1)
    ids = ids_ref[:, :1]
    onehot = jnp.where(ids == code_row, 1.0, 0.0).astype(BF16)
    fill = jnp.where(ids < 0, mask_ref[...].astype(F32), 0.0)
    out_ref[...] = (dot(onehot, table_ref[...]) + fill).astype(BF16)


def own_term(ids, mask, table, tile):
    frames = ids.shape[0]
    codes, width = table.shape
    row_block = lambda i: (i, 0)
    return pl.pallas_call(
        own_term_kernel,
        grid=(frames // tile,),
        in_specs=[
            pl.BlockSpec((tile, 1), row_block),
            pl.BlockSpec((1, width), lambda i: (0, 0)),
            pl.BlockSpec((codes, width), lambda i: (0, 0)),
        ],
        out_specs=pl.BlockSpec((tile, width), row_block),
        out_shape=jax.ShapeDtypeStruct((frames, width), BF16),
        compiler_params=grant(14),
        cost_estimate=pl.CostEstimate(
            flops=2 * frames * codes * width, bytes_accessed=2**22, transcendentals=0
        ),
        name="own_term",
    )(ids, mask, table)


def project_kernel(others, chunks, scale, ids_ref, mask_ref, own_ref, *refs):
    halves, pieces = refs[: 2 * others], refs[2 * others : 2 * others + 4 * chunks]
    embedded_ref, queries_ref, keys_ref, values_ref = refs[2 * others + 4 * chunks :][:4]
    tables, weights = refs[2 * others + 4 * chunks + 4 :]
    codes = tables.shape[0] // others
    half = codes // 2
    core = lax.rem(lax.axis_index(DP), 2)

    @pl.when(pl.program_id(0) == 0)
    def _():
        for index, source in enumerate(halves):
            side = core if index % 2 == 0 else 1 - core
            place = pl.multiple_of((index // 2) * codes + side * half, half)
            tables[pl.ds(place, half), :] = source[:half, :]
        columns = pieces[0].shape[-1]
        for chunk in range(chunks):
            lanes = slice(chunk * columns, (chunk + 1) * columns)
            for matrix in range(weights.shape[0]):
                some = [ref.at[:, matrix] for ref in pieces[4 * chunk : 4 * chunk + 4]]
                place_pieces(some, weights.at[matrix], lanes)

    code_row = lax.broadcasted_iota(jnp.int32, (1, codes), 1)
    part = ids_ref.shape[0] // 2
    rows = [slice(sub * part, (sub + 1) * part) for sub in range(2)]
    totals = []
    for r in rows:
        total = own_ref[r, :].astype(F32)
        for level in range(others):
            ids = ids_ref[r, level : level + 1]
            onehot = jnp.where(ids == code_row, 1.0, 0.0).astype(BF16)
            total = total + dot(onehot, tables[level * codes : (level + 1) * codes, :])
            fill = mask_ref[level : level + 1, :].astype(F32)
            total = total + jnp.where(ids < 0, fill, 0.0)
        totals.append(total)
    for r, total in zip(rows, totals):
        embedded_ref[r, :] = total
        normed = layer_norm(total).astype(BF16)
        queries_ref[r, :] = (dot(normed, weights[0]) * scale).astype(BF16)
        keys_ref[r, :] = dot(normed, weights[1]).astype(BF16)
        values_ref[r, :] = dot(normed, weights[2]).astype(BF16)


def embed_and_project(ids, masks, own, halves, half, pieces, scale, tile):
    frames, others = ids.shape
    width = own.shape[1]
    chunks = len(pieces)
    _, three, _, columns = pieces[0][0].shape
    columns *= chunks
    row_block = lambda i: (i, 0)
    return pl.pallas_call(
        functools.partial(project_kernel, others, chunks, scale),
        grid=(frames // tile,),
        in_specs=[
            pl.BlockSpec((tile, others), row_block),
            pl.BlockSpec(masks.shape, lambda i: (0, 0)),
            pl.BlockSpec((tile, width), row_block),
        ]
        + [WHOLE] * (2 * others + 4 * chunks),
        out_specs=[pl.BlockSpec((tile, width), row_block)]
        + [pl.BlockSpec((tile, columns), row_block)] * 3,
        out_shape=[jax.ShapeDtypeStruct((frames, width), F32)]
        + [jax.ShapeDtypeStruct((frames, columns), BF16)] * 3,
        scratch_shapes=[
            pltpu.VMEM((2 * others * half, width), BF16),
            pltpu.VMEM((three, width, columns), BF16),
        ],
        compiler_params=grant(24 if others == 1 else 60),
        cost_estimate=pl.CostEstimate(
            flops=2 * frames * width * (2 * half * others + three * columns),
            bytes_accessed=20 * 2**20,
            transcendentals=0,
        ),
        name="project",
    )(ids, masks, own, *halves, *[piece for chunk in pieces for piece in chunk])


def attention_kernel(head_dim, quarter, queries_ref, keys_ref, values_ref, out_ref):
    width = out_ref.shape[1]
    lanes = pl.ds(pl.multiple_of(pl.program_id(0) * width, width), width)
    queries, keys, values = queries_ref[quarter, lanes], keys_ref[:, lanes], values_ref[:, lanes]
    lane = lax.broadcasted_iota(jnp.int32, (1, 2 * head_dim), 1)
    first = lane < head_dim
    owns = (first, lane >= head_dim)
    scores = [dot_t(jnp.where(own, queries, jnp.zeros_like(queries)), keys) for own in owns]
    sums = []
    for own, score in zip(owns, scores):
        blocks = [score[:, at : at + 128] for at in range(0, score.shape[1], 128)]
        top = functools.reduce(jnp.maximum, blocks)
        top = jnp.max(top, axis=1, keepdims=True)
        weights = jnp.exp2(score - top).astype(BF16)
        sums.append(dot(weights, jnp.where(own, values, jnp.ones_like(values))))
    mixed = jnp.where(first, sums[0], sums[1])
    total = pltpu.roll(jnp.where(first, sums[1], sums[0]), head_dim, 1)
    out_ref[...] = (mixed / total).astype(BF16)


def attend(queries, keys, values, quarter, tile, head_dim):
    frames, columns = queries.shape
    width = 2 * head_dim
    return pl.pallas_call(
        functools.partial(attention_kernel, head_dim, slice(quarter * tile, (quarter + 1) * tile)),
        grid=(columns // width,),
        in_specs=[WHOLE] * 3,
        out_specs=pl.BlockSpec((tile, width), lambda p: (0, p)),
        out_shape=jax.ShapeDtypeStruct((tile, columns), BF16),
        compiler_params=grant(20),
        cost_estimate=pl.CostEstimate(
            flops=16 * tile * frames * columns, bytes_accessed=2**22, transcendentals=0
        ),
        name="attend",
    )(queries, keys, values)


def gate_kernel(quarters, groups, width, embedded_ref, *refs):
    att_refs = refs[: quarters * groups]
    late = refs[quarters * groups :][:8]
    after_ref, gated_ref, attended, packed = refs[quarters * groups + 8 :]
    step = pl.program_id(0)

    @pl.when(step == 0)
    def _():
        place_pieces(late[:4], packed, slice(0, 2 * width))
        place_pieces(late[4:], packed, slice(2 * width, 3 * width))

    piece = att_refs[0].shape[1]
    for quarter in range(quarters):

        @pl.when(step == quarter)
        def _():
            for group in range(groups):
                attended[:, group * piece : (group + 1) * piece] = att_refs[quarter * groups + group][...]

    part = embedded_ref.shape[0] // 2
    rows = [slice(sub * part, (sub + 1) * part) for sub in range(2)]
    afters = [embedded_ref[r, :] + dot_t(attended[r, :], packed[:, :width]) for r in rows]
    linears = []
    for r, after in zip(rows, afters):
        after_ref[r, :] = after
        linears.append(dot(layer_norm(after).astype(BF16), packed[:, width:]))
    for r, linear in zip(rows, linears):
        gated_ref[r, :] = (linear[:, :width] * gate_of(linear[:, width:])).astype(BF16)


def gate(embedded, attended, late, first, tile):
    width = embedded.shape[1]
    quarters, groups = len(attended), len(attended[0])
    flat = [part for parts in attended for part in parts]
    rows = quarters * tile
    return pl.pallas_call(
        functools.partial(gate_kernel, quarters, groups, width),
        grid=(quarters,),
        in_specs=[pl.BlockSpec((tile, width), lambda i: (first + i, 0))]
        + [pl.BlockSpec(part.shape, lambda i: (0, 0)) for part in flat]
        + [WHOLE] * len(late),
        out_specs=[pl.BlockSpec((tile, width), lambda i: (i, 0))] * 2,
        out_shape=[
            jax.ShapeDtypeStruct((rows, width), F32),
            jax.ShapeDtypeStruct((rows, width), BF16),
        ],
        scratch_shapes=[
            pltpu.VMEM((tile, width), BF16),
            pltpu.VMEM((width, 3 * width), BF16),
        ],
        compiler_params=grant(22),
        cost_estimate=pl.CostEstimate(
            flops=6 * rows * width * width, bytes_accessed=12 * 2**20, transcendentals=0
        ),
        name="gate",
    )(embedded, *flat, *late)


def finish_kernel(tiles, halves, *refs):
    gated_refs, after_refs = refs[: 3 * halves], refs[3 * halves : 4 * halves]
    late = refs[4 * halves :][:4]
    depth_ref, head, out_ref, window, residual, project = refs[4 * halves + 4 :]
    step = pl.program_id(0)
    tile, width = residual.shape
    taps = depth_ref.shape[0]
    edge = 8

    @pl.when(step == 0)
    def _():
        place_pieces(late, project, slice(None))

    per_half = tiles // halves
    for half in range(halves):
        before_ref, here_ref, next_ref = gated_refs[3 * half : 3 * half + 3]

        @pl.when(step // per_half == half)
        def _():
            window[edge : edge + tile, :] = here_ref[...].astype(F32)
            residual[...] = after_refs[half][...]

        @pl.when((step > 0) & ((step - 1) // per_half == half))
        def _():
            window[:edge, :] = before_ref[...].astype(F32)[-edge:, :]

        @pl.when((step < tiles - 1) & ((step + 1) // per_half == half))
        def _():
            window[edge + tile :, :] = next_ref[...].astype(F32)[:edge, :]

    @pl.when(step == 0)
    def _():
        window[:edge, :] = jnp.zeros((edge, width), F32)

    @pl.when(step == tiles - 1)
    def _():
        window[edge + tile :, :] = jnp.zeros((edge, width), F32)

    part = tile // SUBS

    def activate(first):
        blocks = []
        for at in range(0, width, 128):
            lanes = slice(at, at + 128)
            near = window[first : first + part + 2 * edge, lanes]
            conv = None
            for tap in range(taps):
                start = edge - taps // 2 + tap
                term = near[start : start + part] * depth_ref[tap : tap + 1, lanes].astype(F32)
                conv = term if conv is None else conv + term
            blocks.append((conv * gate_of(conv)).astype(BF16))
        return jnp.concatenate(blocks, axis=1)

    activated = activate(0)
    waiting = None
    for sub in range(SUBS + 1):
        mixed = None
        if sub < SUBS:
            mixed = dot(activated, project[...])
            if sub + 1 < SUBS:
                activated = activate((sub + 1) * part)
        if sub > 0:
            r = slice((sub - 1) * part, sub * part)
            normed = layer_norm(residual[r, :] + waiting).astype(BF16)
            out_ref[r, :] = dot(normed, head[...]).astype(BF16)
        waiting = mixed


def finish(gated, after, late, w_depth, head, tile):
    halves = len(gated)
    half_rows, width = gated[0].shape
    codes = head.shape[1]
    frames = halves * half_rows
    tiles = frames // tile
    per_half = half_rows // tile
    strip = STRIP
    per_tile = tile // strip

    def clip(index, half):
        return jnp.clip(index - half * per_half, 0, per_half - 1)

    specs = []
    for half in range(halves):
        specs += [
            pl.BlockSpec((strip, width), lambda i, half=half: (clip(i - 1, half) * per_tile + per_tile - 1, 0)),
            pl.BlockSpec((tile, width), lambda i, half=half: (clip(i, half), 0)),
            pl.BlockSpec((strip, width), lambda i, half=half: (clip(i + 1, half) * per_tile, 0)),
        ]
    for half in range(halves):
        specs.append(pl.BlockSpec((tile, width), lambda i, half=half: (clip(i, half), 0)))
    return pl.pallas_call(
        functools.partial(finish_kernel, tiles, halves),
        grid=(tiles,),
        in_specs=specs + [WHOLE] * 4 + [pl.BlockSpec(w_depth.shape, lambda i: (0, 0)), WHOLE],
        out_specs=pl.BlockSpec((tile, codes), lambda i: (i, 0)),
        out_shape=jax.ShapeDtypeStruct((frames, codes), BF16),
        scratch_shapes=[
            pltpu.VMEM((tile + 16, width), F32),
            pltpu.VMEM((tile, width), F32),
            pltpu.VMEM((width, width), BF16),
        ],
        compiler_params=grant(22),
        cost_estimate=pl.CostEstimate(
            flops=2 * frames * width * (width + codes), bytes_accessed=20 * 2**20, transcendentals=0
        ),
        name="finish",
    )(*[g for half in gated for g in (half, half, half)], *after, *late, w_depth, head)


def body(
    token_ids,
    decoded_mask,
    levels_done,
    code_tables,
    mask_vectors,
    w_qkv,
    w_out,
    w_expand,
    w_depth,
    w_project,
    level_heads,
):
    return step(
        token_ids[0, 0], decoded_mask[0, 0], levels_done[0], code_tables[0], mask_vectors,
        w_qkv, w_out, w_expand, w_depth, w_project, level_heads[0],
    )[None, None]


def step(
    token_ids, decoded_mask, done, table, own_mask, w_qkv, w_out, w_expand, w_depth, w_project, head,
):
    groups = lax.axis_size(LEVEL)
    level_index = lax.axis_index(LEVEL)
    frames = token_ids.shape[0]
    codes, width = table.shape
    head_dim = width // HEADS
    half = codes // 2
    core = lax.rem(lax.axis_index(DP), 2)
    backs = range(1, groups)

    own_out = w_out.T
    columns = own_out.shape[1]
    outs = [own_out] + [from_level(own_out, back) for back in backs]
    late_shards = (
        jnp.concatenate(outs + [w_expand[:, :width]], axis=1),
        jnp.concatenate([w_expand[:, width:], w_project], axis=1),
    )

    use_token = (level_index < done) | ((level_index == done) & (decoded_mask == 1))
    own_ids = jnp.where(use_token, token_ids, -1)
    ids = jnp.stack([from_level(own_ids, back) for back in backs], axis=1)

    mine = lax.dynamic_slice_in_dim(table, core * half, half, 0)
    mine = jnp.concatenate([mine, jnp.broadcast_to(own_mask, (STRIP, width))], axis=0)
    halves, masks = [], []
    for back in backs:
        landed = from_level(mine, back)
        masks.append(landed[half : half + 1])
        halves += [landed, swap(landed, 1)]
    pieces = []
    chunk = columns // CHUNKS if columns % (128 * CHUNKS) == 0 else columns
    for at in range(columns // chunk):
        near = gather_outer(w_qkv[:, :, at * chunk : (at + 1) * chunk])
        pieces.append(gather_chip_pairs(near))
    late = [gather_chip_pairs(gather_outer(late_shards[0]))]
    near = gather_outer(late_shards[1])
    for at in range(2):
        part = [piece[:, at * width : (at + 1) * width] for piece in near]
        late.append(gather_chip_pairs(part))

    tile = frames // QUARTERS
    own = own_term(own_ids[:, None], own_mask, table, tile)
    scale = head_dim ** (-0.5) * LOG2E
    embedded, queries, keys, values = embed_and_project(
        ids, jnp.concatenate(masks), own, halves, half, pieces, scale, tile
    )

    attended = []
    for quarter in range(QUARTERS):
        part = attend(queries, keys, values, quarter, tile, head_dim)
        attended.append([part] + [from_level(part, back) for back in backs])
    after, gated = [], []
    per_half = QUARTERS // 2
    for part in range(2):
        some = attended[part * per_half : (part + 1) * per_half]
        result = gate(embedded, some, late[0] + late[1], part * per_half, tile)
        after.append(result[0])
        gated.append(result[1])
    return finish(gated, after, late[2], w_depth, head, tile)


def solution(mesh):
    return jax.shard_map(
        body,
        mesh=mesh,
        in_specs=(
            P(DP, LEVEL, None),
            P(DP, LEVEL, None),
            P(DP),
            P(LEVEL, None, None),
            P(LEVEL, None),
            P(None, DP, LEVEL),
            P(LEVEL, DP),
            P(DP, None),
            P(),
            P(DP, None),
            P(LEVEL, None, None),
        ),
        out_specs=P(DP, LEVEL, None, None),
        check_vma=False,
    )
```
